32 devices in a mesh: aux: 4 (over z), orb: 8 (over y, x, core).
Axes of the slice: x: 2, y: 2, z: 4, core: 2. Of those that a mesh axis runs over, the one named last changes fastest.
Arguments:
- half: bfloat16 [64, 384, 3072], P('aux', 'orb'), may hold values from -1.25 to 1.25
- metric: bfloat16 [64, 64], P('aux'), may hold values from -1 to 2
- survive: int32 [4, 16, 24], P('aux', 'orb'), may hold values 0 or 1
Outputs:
- exchange_k: float32 [3072, 3072], P('orb', 'aux')
The draws below stay inside these ranges and needn't reach their ends.
All inputs are finite; a program needn't handle non-finite values. No bound on the sum of `survive` on one device may be relied on, other than what follows from the above.
Results may differ from the reference program's by a relative error of at most 0.00098.
Values may be sent and summed in bfloat16 or wider, within the bound.
A program may use at most 128 MiB of HBM per device.

```python
import jax
import jax.numpy as jnp
from jax import lax

NOCC = 384
OCCB = 24
NAO = 3072
AOBLK = 128
NAUX = 64
N_AUX = 4


def draw_metric(key, part):
    first_key = jax.random.fold_in(key, 11)
    second_key = jax.random.fold_in(key, 12)
    spread = jax.random.normal(first_key, (NAUX, NAUX), jnp.float32) * (0.6 / NAUX ** 0.5)
    diagonal_part = jax.random.uniform(second_key, (NAUX,), jnp.float32, 0.9, 1.1)
    return (spread + jnp.diag(diagonal_part)).astype(jnp.bfloat16)


def set_ends(entries, own_key, low, largest):
    shape = entries.shape
    place = [jax.random.randint(jax.random.fold_in(own_key, axis), (), 0, shape[axis]) for axis in range(len(shape))]
    entries = entries.at[tuple(place)].set(low)
    longest = shape.index(max(shape))
    place[longest] = (place[longest] + 1) % shape[longest]
    return entries.at[tuple(place)].set(largest)


def steps_of(key, shape, cuts, low, largest):
    def one(axis_at, shards_of):
        draws = jax.random.uniform(jax.random.fold_in(jax.random.fold_in(key, 6), axis_at), (shards_of,), jnp.float32, low / len(cuts), largest / len(cuts))
        return jnp.repeat(jnp.exp(draws), shape[axis_at] // shards_of).reshape((-1,) + (1,) * (len(shape) - axis_at - 1))

    level = one(*cuts[0])
    for cut in cuts[1:]:
        level = level * one(*cut)
    return level


def bell_draw(key, shape, scale, most, shards=(), kind=jnp.bfloat16):
    factor_of = steps_of(key, shape, shards, -0.22, 0.18) if shards else 1.0
    values = jax.random.normal(key, shape, jnp.float32) * scale * factor_of
    return jnp.minimum(jnp.maximum(values, -most), most).astype(kind)


def setup_inputs(seed: int = 0) -> dict:
    key_of = jax.random.split(jax.random.key(seed), 4)
    half = bell_draw(key_of[0], (NAUX, NOCC, NAO), ((NAUX * NOCC) ** -0.25), 1.25, ((0, 4), (1, 8)))
    metric = draw_metric(jax.random.fold_in(key_of[3], 71), 0)
    survive = set_ends((jax.random.randint(key_of[2], (N_AUX, NOCC // OCCB, NAO // AOBLK), 0, 3) < 2).astype(jnp.int32), jax.random.fold_in(key_of[2], 1), 0, 1)
    return dict(half=half, metric=metric, survive=survive)


def reference(half, metric, survive):
    blocks_aux, blocks_occ, blocks_ao = survive.shape
    aux_count, occ_count, ao_count = half.shape
    gate = survive.astype(jnp.bfloat16)
    shaped = half.reshape(blocks_aux, aux_count // blocks_aux, blocks_occ, occ_count // blocks_occ, blocks_ao, ao_count // blocks_ao)
    masked = (shaped * gate[:, None, :, None, :, None]).reshape(aux_count, occ_count, ao_count)
    occ_width = occ_count // blocks_occ

    def accumulate(totals, block_index):
        occ_rows = lax.dynamic_slice_in_dim(masked, block_index * occ_width, occ_width, 1)
        fitted = jnp.dot(metric, occ_rows.reshape(aux_count, -1), preferred_element_type=jnp.float32)
        fitted = fitted.astype(jnp.bfloat16).reshape(-1, ao_count)
        update = lax.dot_general(fitted, fitted, (((0,), (0,)), ((), ())), preferred_element_type=jnp.float32)
        return totals + update, None

    exchange_k, _ = lax.scan(accumulate, jnp.zeros((ao_count, ao_count), jnp.float32), jnp.arange(blocks_occ, dtype=jnp.int32))
    return exchange_k
```

```python
import functools

import jax
import jax.numpy as jnp
from jax import lax
from jax.experimental import pallas as pl
from jax.experimental.pallas import tpu as pltpu
from jax.sharding import PartitionSpec as P

MESH = pl.DeviceIdType.MESH
F32 = jnp.float32


def gated(half, survive):
    aux_local, occ_local, ao_count = half.shape
    blocks_aux, blocks_occ, blocks_ao = survive.shape
    gate = survive.astype(jnp.bfloat16)
    shaped = half.reshape(
        blocks_aux, aux_local, blocks_occ, occ_local // blocks_occ, blocks_ao, ao_count // blocks_ao
    )
    return (shaped * gate[:, None, :, None, :, None]).reshape(aux_local, occ_local, ao_count)


def plain(half, metric, survive):
    aux_local, occ_local, ao_count = half.shape
    portion = lax.all_gather(gated(half, survive), "aux", axis=0, tiled=True)
    fit_total = jnp.dot(metric, portion.reshape(portion.shape[0], -1), preferred_element_type=F32)
    fitted = fit_total.astype(jnp.bfloat16).reshape(aux_local, occ_local, ao_count)
    group_width = ao_count // lax.axis_size("orb")
    row_start = lax.axis_index("orb") * group_width
    flat_rows = lax.all_gather(fitted, "orb", axis=1, tiled=True).reshape(-1, ao_count)
    left_rows = lax.dynamic_slice_in_dim(flat_rows, row_start, group_width, 1)
    partial_k = lax.dot_general(
        left_rows, flat_rows, (((0,), (0,)), ((), ())), preferred_element_type=F32
    )
    return lax.psum_scatter(partial_k, "aux", scatter_dimension=1, tiled=True)


def kernel(
    m_ref, kron_ref, out_ref, held, fit, left, acc, peer, tile, via, last,
    zs, zr, xs, xr, ys, yr, fs, fr, ps, pr, rs, rr,
):
    z = lax.axis_index("aux")
    orb = lax.axis_index("orb")
    n_aux = m_ref.shape[0]
    unit = m_ref.shape[1]
    ao = m_ref.shape[2]
    chip = orb // 2
    core = orb % 2
    pair_rows = acc.shape[0]
    rows = pair_rows // 2
    cols = out_ref.shape[1]
    half_rows = rows // 2
    x_peer = orb + 2 - 4 * (chip % 2)
    y_peer = orb + 4 - 8 * (chip // 2)
    partner = orb + 1 - 2 * core
    up, down, far = (z + 1) % n_aux, (z + n_aux - 1) % n_aux, (z + 2) % n_aux

    barrier = pltpu.get_barrier_semaphore()
    for a in (up, down, far):
        pl.semaphore_signal(barrier, inc=1, device_id={"aux": a, "orb": orb}, device_id_type=MESH)
    for o in (x_peer, y_peer, partner):
        pl.semaphore_signal(barrier, inc=1, device_id={"aux": z, "orb": o}, device_id_type=MESH)
    pl.semaphore_wait(barrier, 6)

    def remote(src, dst, send, recv, a, o):
        return pltpu.make_async_remote_copy(
            src_ref=src, dst_ref=dst, send_sem=send, recv_sem=recv,
            device_id={"aux": a, "orb": o}, device_id_type=MESH,
        )

    def span(s):
        return pl.ds(pl.multiple_of(s * unit, unit), unit)

    def source(d):
        return (z + n_aux - d) % n_aux

    spread = {}
    for d in (1, 3, 2):
        there = (z + d) % n_aux
        spread[d] = remote(m_ref.at[there], held.at[0, span(z)], zs.at[d], zr.at[d], there, orb)
        spread[d].start()

    to_x, to_y, onward = {}, {}, {}

    def share(d):
        own = span(source(d))
        if d:
            spread[d].wait_recv()
        block = held.at[0, own] if d else m_ref.at[z]
        to_x[d] = remote(block, held.at[1, own], xs.at[d], xr.at[d], z, x_peer)
        to_y[d] = remote(block, held.at[2, own], ys.at[d], yr.at[d], z, y_peer)
        to_x[d].start()
        to_y[d].start()

    def forward(d, from_x):
        own = span(source(d))
        if from_x:
            to_x[d].wait_recv()
            onward[d] = remote(held.at[1, own], held.at[3, own], fs.at[d], fr.at[d], z, y_peer)
        else:
            to_y[d].wait_recv()
            onward[d] = remote(held.at[2, own], held.at[3, own], fs.at[d], fr.at[d], z, x_peer)
        onward[d].start()

    step = 512
    mine = pl.ds(pl.multiple_of(chip * pair_rows, pair_rows), pair_rows)

    def contract(slot, first):
        @pl.loop(0, ao // step)
        def _(t):
            at = pl.ds(pl.multiple_of(t * step, step), step)
            fit[:, at] = jnp.dot(
                kron_ref[...], held[slot, :, at], preferred_element_type=F32
            ).astype(fit.dtype)

        left[...] = fit[:, mine].T

        @pl.loop(0, ao // step)
        def _(t):
            at = pl.ds(pl.multiple_of(t * step, step), step)
            more = jnp.dot(left[...], fit[:, at], preferred_element_type=F32)
            acc[:, at] = more if first else acc[:, at] + more

    share(0)
    held[0, span(z), :] = m_ref[z]
    share(1)
    share(3)
    forward(0, True)
    share(2)
    forward(1, False)
    contract(0, True)
    forward(3, True)
    to_x[1].wait_recv()
    to_x[2].wait_recv()
    contract(1, False)
    forward(2, False)
    to_y[0].wait_recv()
    to_y[3].wait_recv()
    contract(2, False)
    for d in range(4):
        onward[d].wait_recv()
    contract(3, False)

    def across(a):
        return pl.ds(pl.multiple_of(a * cols, cols), cols)

    my_rows = pl.ds(pl.multiple_of(core * rows, rows), rows)
    other_rows = pl.ds(pl.multiple_of((1 - core) * rows, rows), rows)
    order = (far, up, down, z)
    swaps = []
    for n, a in enumerate(order):
        swap = remote(acc.at[other_rows, across(a)], peer.at[n], ps.at[n], pr.at[n], z, partner)
        swap.start()
        swaps.append(swap)

    low, high = pl.ds(0, half_rows), pl.ds(half_rows, half_rows)

    def settle(n):
        swaps[n].wait_recv()
        tile[n] = acc[my_rows, across(order[n])] + peer[n]

    settle(0)
    far_up = remote(tile.at[0, low], via.at[0], rs.at[0], rr.at[0], up, orb)
    far_down = remote(tile.at[0, high], via.at[1], rs.at[1], rr.at[1], down, orb)
    far_up.start()
    far_down.start()
    settle(1)
    near_up = remote(tile.at[1, high], last.at[0, high], rs.at[2], rr.at[2], up, orb)
    near_up.start()
    settle(2)
    near_down = remote(tile.at[2, low], last.at[1, low], rs.at[3], rr.at[3], down, orb)
    near_down.start()
    settle(3)
    far_up.wait_recv()
    tile[1, low] += via[0]
    sum_up = remote(tile.at[1, low], last.at[0, low], rs.at[4], rr.at[4], up, orb)
    sum_up.start()
    far_down.wait_recv()
    tile[2, high] += via[1]
    sum_down = remote(tile.at[2, high], last.at[1, high], rs.at[5], rr.at[5], down, orb)
    sum_down.start()
    for copy in (near_up, near_down, sum_up, sum_down):
        copy.wait_recv()
    out_ref[...] = tile[3] + last[0] + last[1]
    for copy in (
        *spread.values(), *to_x.values(), *to_y.values(), *onward.values(), *swaps,
        far_up, far_down, near_up, near_down, sum_up, sum_down,
    ):
        copy.wait_send()


def direct(half, metric, survive):
    aux_local, occ_local, ao = half.shape
    n_aux, n_orb = lax.axis_size("aux"), lax.axis_size("orb")
    part = occ_local // n_aux
    blocks = gated(half, survive).reshape(aux_local, n_aux, part, ao)
    blocks = blocks.transpose(1, 0, 2, 3).reshape(n_aux, aux_local * part, ao)
    whole_metric = lax.all_gather(metric, "aux", axis=0, tiled=True)
    kron = jnp.kron(whole_metric, jnp.eye(part, dtype=metric.dtype))
    depth = kron.shape[0]
    rows, cols = ao // n_orb, ao // n_aux
    dma = pltpu.SemaphoreType.DMA
    bf16 = jnp.bfloat16
    return pl.pallas_call(
        kernel,
        out_shape=jax.ShapeDtypeStruct((rows, cols), F32),
        in_specs=[pl.BlockSpec(memory_space=pltpu.VMEM)] * 2,
        out_specs=pl.BlockSpec(memory_space=pltpu.VMEM),
        scratch_shapes=[
            pltpu.VMEM((4, depth, ao), bf16),
            pltpu.VMEM((depth, ao), bf16),
            pltpu.VMEM((2 * rows, depth), bf16),
            pltpu.VMEM((2 * rows, ao), F32),
            pltpu.VMEM((4, rows, cols), F32),
            pltpu.VMEM((4, rows, cols), F32),
            pltpu.VMEM((2, rows // 2, cols), F32),
            pltpu.VMEM((2, rows, cols), F32),
        ]
        + [dma((4,))] * 10
        + [dma((6,))] * 2,
        compiler_params=pltpu.CompilerParams(
            collective_id=0, has_side_effects=True, vmem_limit_bytes=66 * 1000 * 1000
        ),
    )(blocks, kron)


def solution(mesh):
    square = mesh.shape["aux"] == 4 and mesh.shape["orb"] == 8
    return jax.shard_map(
        direct if square else plain,
        mesh=mesh,
        in_specs=(P("aux", "orb", None), P("aux", None), P("aux", "orb", None)),
        out_specs=P("orb", "aux"),
        check_vma=False,
    )
```

```python
import functools

import jax
import jax.numpy as jnp
from jax import lax
from jax.experimental import pallas as pl
from jax.experimental.pallas import tpu as pltpu
from jax.sharding import PartitionSpec as P

MESH = pl.DeviceIdType.MESH
F32 = jnp.float32


def gated(half, survive):
    aux_local, occ_local, ao_count = half.shape
    blocks_aux, blocks_occ, blocks_ao = survive.shape
    gate = survive.astype(jnp.bfloat16)
    shaped = half.reshape(
        blocks_aux, aux_local, blocks_occ, occ_local // blocks_occ, blocks_ao, ao_count // blocks_ao
    )
    return (shaped * gate[:, None, :, None, :, None]).reshape(aux_local, occ_local, ao_count)


def plain(half, metric, survive):
    aux_local, occ_local, ao_count = half.shape
    portion = lax.all_gather(gated(half, survive), "aux", axis=0, tiled=True)
    fit_total = jnp.dot(metric, portion.reshape(portion.shape[0], -1), preferred_element_type=F32)
    fitted = fit_total.astype(jnp.bfloat16).reshape(aux_local, occ_local, ao_count)
    group_width = ao_count // lax.axis_size("orb")
    row_start = lax.axis_index("orb") * group_width
    flat_rows = lax.all_gather(fitted, "orb", axis=1, tiled=True).reshape(-1, ao_count)
    left_rows = lax.dynamic_slice_in_dim(flat_rows, row_start, group_width, 1)
    partial_k = lax.dot_general(
        left_rows, flat_rows, (((0,), (0,)), ((), ())), preferred_element_type=F32
    )
    return lax.psum_scatter(partial_k, "aux", scatter_dimension=1, tiled=True)


def kernel(
    aux_local, m_ref, metric_ref, out_ref, held, fit, left, acc, peer, tile, via, last, whole, kron_ref,
    gs, gr, zs, zr, xs, xr, ys, yr, fs, fr, ps, pr, rs, rr,
):
    z = lax.axis_index("aux")
    orb = lax.axis_index("orb")
    n_aux = m_ref.shape[0]
    unit = m_ref.shape[1]
    ao = m_ref.shape[2]
    chip = orb // 2
    core = orb % 2
    pair_rows = acc.shape[0]
    rows = pair_rows // 2
    cols = out_ref.shape[1]
    half_rows = rows // 2
    x_peer = orb + 2 - 4 * (chip % 2)
    y_peer = orb + 4 - 8 * (chip // 2)
    partner = orb + 1 - 2 * core
    up, down, far = (z + 1) % n_aux, (z + n_aux - 1) % n_aux, (z + 2) % n_aux

    barrier = pltpu.get_barrier_semaphore()
    for a in (up, down, far):
        pl.semaphore_signal(barrier, inc=1, device_id={"aux": a, "orb": orb}, device_id_type=MESH)
    for o in (x_peer, y_peer, partner):
        pl.semaphore_signal(barrier, inc=1, device_id={"aux": z, "orb": o}, device_id_type=MESH)
    pl.semaphore_wait(barrier, 6)

    def remote(src, dst, send, recv, a, o):
        return pltpu.make_async_remote_copy(
            src_ref=src, dst_ref=dst, send_sem=send, recv_sem=recv,
            device_id={"aux": a, "orb": o}, device_id_type=MESH,
        )

    def span(s):
        return pl.ds(pl.multiple_of(s * unit, unit), unit)

    def source(d):
        return (z + n_aux - d) % n_aux

    metric_rows = pl.ds(pl.multiple_of(z * aux_local, aux_local), aux_local)
    gather = []
    for d in (1, 3, 2):
        copy = remote(metric_ref, whole.at[metric_rows], gs.at[d], gr.at[d], (z + d) % n_aux, orb)
        copy.start()
        gather.append(copy)
    spread = {}
    for d in (1, 3, 2):
        there = (z + d) % n_aux
        spread[d] = remote(m_ref.at[there], held.at[0, span(z)], zs.at[d], zr.at[d], there, orb)
        spread[d].start()

    to_x, to_y, onward = {}, {}, {}

    def share(d):
        own = span(source(d))
        if d:
            spread[d].wait_recv()
        block = held.at[0, own] if d else m_ref.at[z]
        to_x[d] = remote(block, held.at[1, own], xs.at[d], xr.at[d], z, x_peer)
        to_y[d] = remote(block, held.at[2, own], ys.at[d], yr.at[d], z, y_peer)
        to_x[d].start()
        to_y[d].start()

    def forward(d, from_x):
        own = span(source(d))
        if from_x:
            to_x[d].wait_recv()
            onward[d] = remote(held.at[1, own], held.at[3, own], fs.at[d], fr.at[d], z, y_peer)
        else:
            to_y[d].wait_recv()
            onward[d] = remote(held.at[2, own], held.at[3, own], fs.at[d], fr.at[d], z, x_peer)
        onward[d].start()

    step = 512
    mine = pl.ds(pl.multiple_of(chip * pair_rows, pair_rows), pair_rows)

    def contract(slot, first):
        @pl.loop(0, ao // step)
        def _(t):
            at = pl.ds(pl.multiple_of(t * step, step), step)
            fit[:, at] = jnp.dot(
                kron_ref[...], held[slot, :, at], preferred_element_type=F32
            ).astype(fit.dtype)

        left[...] = fit[:, mine].T

        @pl.loop(0, ao // step)
        def _(t):
            at = pl.ds(pl.multiple_of(t * step, step), step)
            more = jnp.dot(left[...], fit[:, at], preferred_element_type=F32)
            acc[:, at] = more if first else acc[:, at] + more

    def build_kron():
        whole[metric_rows, :] = metric_ref[...]
        for copy in gather:
            copy.wait_recv()
        depth, width = kron_ref.shape[0], whole.shape[1]

        def aux_of(r):
            return lax.div(r, unit) * aux_local + lax.rem(r, aux_local)

        def orbital_of(r):
            return lax.div(lax.rem(r, unit), aux_local)

        i32, bf16 = jnp.int32, kron_ref.dtype
        by_row = aux_of(lax.broadcasted_iota(i32, (width, depth), 1))
        pick = jnp.where(by_row == lax.broadcasted_iota(i32, (width, depth), 0), 1.0, 0.0)
        spread_cols = jnp.dot(whole[...], pick.astype(bf16), preferred_element_type=F32).astype(bf16)
        by_col = aux_of(lax.broadcasted_iota(i32, (depth, whole.shape[0]), 0))
        take = jnp.where(by_col == lax.broadcasted_iota(i32, (depth, whole.shape[0]), 1), 1.0, 0.0)
        both = jnp.dot(take.astype(bf16), spread_cols, preferred_element_type=F32)
        same = orbital_of(lax.broadcasted_iota(i32, (depth, depth), 0)) == orbital_of(
            lax.broadcasted_iota(i32, (depth, depth), 1)
        )
        kron_ref[...] = jnp.where(same, both, 0.0).astype(bf16)

    share(0)
    held[0, span(z), :] = m_ref[z]
    build_kron()
    share(1)
    share(3)
    forward(0, True)
    share(2)
    forward(1, False)
    contract(0, True)
    forward(3, True)
    to_x[1].wait_recv()
    to_x[2].wait_recv()
    contract(1, False)
    forward(2, False)
    to_y[0].wait_recv()
    to_y[3].wait_recv()
    contract(2, False)
    for d in range(4):
        onward[d].wait_recv()
    contract(3, False)

    def across(a):
        return pl.ds(pl.multiple_of(a * cols, cols), cols)

    my_rows = pl.ds(pl.multiple_of(core * rows, rows), rows)
    other_rows = pl.ds(pl.multiple_of((1 - core) * rows, rows), rows)
    order = (far, up, down, z)
    swaps = []
    for n, a in enumerate(order):
        swap = remote(acc.at[other_rows, across(a)], peer.at[n], ps.at[n], pr.at[n], z, partner)
        swap.start()
        swaps.append(swap)

    low, high = pl.ds(0, half_rows), pl.ds(half_rows, half_rows)

    def settle(n):
        swaps[n].wait_recv()
        tile[n] = acc[my_rows, across(order[n])] + peer[n]

    settle(0)
    far_up = remote(tile.at[0, low], via.at[0], rs.at[0], rr.at[0], up, orb)
    far_down = remote(tile.at[0, high], via.at[1], rs.at[1], rr.at[1], down, orb)
    far_up.start()
    far_down.start()
    settle(1)
    near_up = remote(tile.at[1, high], last.at[0, high], rs.at[2], rr.at[2], up, orb)
    near_up.start()
    settle(2)
    near_down = remote(tile.at[2, low], last.at[1, low], rs.at[3], rr.at[3], down, orb)
    near_down.start()
    settle(3)
    far_up.wait_recv()
    tile[1, low] += via[0]
    sum_up = remote(tile.at[1, low], last.at[0, low], rs.at[4], rr.at[4], up, orb)
    sum_up.start()
    far_down.wait_recv()
    tile[2, high] += via[1]
    sum_down = remote(tile.at[2, high], last.at[1, high], rs.at[5], rr.at[5], down, orb)
    sum_down.start()
    for copy in (near_up, near_down, sum_up, sum_down):
        copy.wait_recv()
    out_ref[...] = tile[3] + last[0] + last[1]
    for copy in (
        *gather, *spread.values(), *to_x.values(), *to_y.values(), *onward.values(), *swaps,
        far_up, far_down, near_up, near_down, sum_up, sum_down,
    ):
        copy.wait_send()


def direct(half, metric, survive):
    aux_local, occ_local, ao = half.shape
    n_aux, n_orb = lax.axis_size("aux"), lax.axis_size("orb")
    part = occ_local // n_aux
    blocks = gated(half, survive).transpose(1, 0, 2).reshape(n_aux, part * aux_local, ao)
    n_fit = n_aux * aux_local
    width = -(-n_fit // 128) * 128
    metric = jnp.pad(metric, ((0, 0), (0, width - n_fit)))
    depth = n_fit * part
    rows, cols = ao // n_orb, ao // n_aux
    dma = pltpu.SemaphoreType.DMA
    bf16 = jnp.bfloat16
    return pl.pallas_call(
        functools.partial(kernel, aux_local),
        out_shape=jax.ShapeDtypeStruct((rows, cols), F32),
        in_specs=[pl.BlockSpec(memory_space=pltpu.VMEM)] * 2,
        out_specs=pl.BlockSpec(memory_space=pltpu.VMEM),
        scratch_shapes=[
            pltpu.VMEM((4, depth, ao), bf16),
            pltpu.VMEM((depth, ao), bf16),
            pltpu.VMEM((2 * rows, depth), bf16),
            pltpu.VMEM((2 * rows, ao), F32),
            pltpu.VMEM((4, rows, cols), F32),
            pltpu.VMEM((4, rows, cols), F32),
            pltpu.VMEM((2, rows // 2, cols), F32),
            pltpu.VMEM((2, rows, cols), F32),
            pltpu.VMEM((n_fit, width), bf16),
            pltpu.VMEM((depth, depth), bf16),
        ]
        + [dma((4,))] * 12
        + [dma((6,))] * 2,
        compiler_params=pltpu.CompilerParams(
            collective_id=0, has_side_effects=True, vmem_limit_bytes=66 * 1000 * 1000
        ),
    )(blocks, metric)


def solution(mesh):
    square = mesh.shape["aux"] == 4 and mesh.shape["orb"] == 8
    return jax.shard_map(
        direct if square else plain,
        mesh=mesh,
        in_specs=(P("aux", "orb", None), P("aux", None), P("aux", "orb", None)),
        out_specs=P("orb", "aux"),
        check_vma=False,
    )
```
